32 devices in a mesh: expert: 8 (over z, y), gate: 4 (over x, core).
Axes of the slice: x: 2, y: 2, z: 4, core: 2. Of those that a mesh axis runs over, the one named last changes fastest.
Arguments:
- samples: bfloat16 [6144, 4096], P('expert', 'gate'), may hold values from -4 to 4
- gate_weight: bfloat16 [4096, 32], P('gate'), may hold values from -1 to 1
- expert_ids: int32 [6144, 2], P('expert'), may hold values from 0 to 31, all different within a row; in each aligned block of 768 rows (0 to 767, 768 to 1535, ...) at most 96 rows name the same one
- pad_mask: int32 [6144], P('expert'), may hold values 0 or 1
- up_weight: bfloat16 [32, 4096, 1024], P(('expert', 'gate')), may hold values from -0.09375 to 0.09375
- down_weight: bfloat16 [32, 1024, 1024], P(('expert', 'gate')), may hold values from -0.1875 to 0.1875
Outputs:
- combined: bfloat16 [6144, 1024], P('expert', 'gate')
The draws below stay inside these ranges and needn't reach their ends.
Inputs may be any that keep to these rules, and one draw needn't show every extreme that they name: `expert_ids`: each sample names two different experts; among the 768 samples of one index of expert no expert is named more than 96 times, a bound that some block reaches.
All inputs are finite; a program needn't handle non-finite values. No bound on the sum of `pad_mask` on one device may be relied on, other than what follows from the above.
Results may differ from the reference program's by a relative error of at most 0.0057.
Values may be sent and summed in bfloat16 or wider, within the bound.
No kernel may reach another device: no remote copies, remote signals or barrier semaphores. Data moves between devices by JAX's collectives and lax.ppermute only.
A program may use at most 128 MiB of HBM per device.

```python
import math
import jax
import jax.numpy as jnp
import numpy as np
from jax import lax

D = 4096
H = 1024
OUT = 1024
ROWS_DEV = 768
EXPERTS = 32
CAP = 96
BATCH = 6144
N_EXPERT = 8


def draw_samples(key, part):
    inner = jax.random.fold_in(key, 3)
    drawn = jnp.clip(jax.random.normal(inner, (BATCH, D), jnp.float32), -4.0, 4.0)
    return drawn.astype(jnp.bfloat16)


def draw_gate_weight(key, part):
    inner = jax.random.fold_in(key, 5)
    spread_key = jax.random.fold_in(key, 6)
    scales = jnp.exp(jax.random.uniform(spread_key, (1, EXPERTS), jnp.float32, jnp.log(0.15), jnp.log(1.5)))
    drawn = jnp.clip(jax.random.normal(inner, (D, EXPERTS), jnp.float32), -4.0, 4.0)
    drawn = drawn * scales / jnp.sqrt(jnp.float32(D))
    return drawn.astype(jnp.bfloat16)


def place_ends(entries, rng, low, high):
    place = [jax.random.randint(jax.random.fold_in(rng, axis), (), 0, length) for axis, length in enumerate(entries.shape)]
    longest = entries.shape.index(max(entries.shape))
    neighbour = place[:longest] + [(place[longest] + 1) % entries.shape[longest]] + place[longest + 1:]
    return entries.at[tuple(place)].set(low).at[tuple(neighbour)].set(high)


def levels(key, extent, cuts, low, largest):
    def one(dim, blocks):
        draws = jax.random.uniform(jax.random.fold_in(jax.random.fold_in(key, 6), dim), (blocks,), jnp.float32, low / len(cuts), largest / len(cuts))
        return jnp.repeat(jnp.exp(draws), extent[dim] // blocks).reshape((-1,) + (1,) * (len(extent) - dim - 1))

    loudness = one(*cuts[0])
    for cut in cuts[1:]:
        loudness = loudness * one(*cut)
    return loudness


def routed_block(rng, own, number, rows, number_of, top, reach, skew):
    order = jax.random.permutation(rng, number_of)
    packed, usual = portions_of(number_of, rows * top, reach, skew, True), portions_of(number_of, rows * top, reach, skew, False)
    places = jnp.arange(number_of)

    def named(sizes, offset_by):
        used = int((sizes > 0).sum())
        fixed = max(1, used // 4)
        moved = fixed + (places - fixed + offset_by * (used - fixed)) % max(1, number_of - fixed)
        return jnp.zeros((number_of,), jnp.int32).at[order[jnp.where(places < fixed, places, moved)]].set(jnp.asarray(sizes, jnp.int32))

    sizes = jnp.where(number % 4 == 0, named(packed, number // 4), named(usual, number - number // 4 - 1))
    mixed = jax.random.permutation(jax.random.fold_in(own, 3), number_of)
    source_of, taker = mixed[0:number_of // 2 * 2:2], mixed[1:number_of // 2 * 2:2]
    room = jnp.minimum(sizes[source_of] - 1, reach - sizes[taker]) // 2
    room = jnp.where((source_of == order[0]) | (taker == order[0]) | (sizes[taker] == 0), 0, jnp.maximum(room, 0))
    moved = jax.random.randint(jax.random.fold_in(own, 4), (number_of // 2,), 0, 1 << 20) % (room + 1)
    sizes = sizes.at[source_of].add(-moved).at[taker].add(moved)
    labels = jnp.searchsorted(jnp.cumsum(sizes), jnp.arange(rows * top), side="right").astype(jnp.int32)
    listing = labels.reshape(top, rows).T
    listing = listing[jax.random.permutation(jax.random.fold_in(own, 1), rows)]
    offset_by = jax.random.randint(jax.random.fold_in(own, 2), (rows, 1), 0, top)
    return jnp.take_along_axis(listing, (jnp.arange(top)[None, :] + offset_by) % top, axis=1)


def portions_of(number_of, total, limit, slope, full):
    weights = [(1 << 20) // math.isqrt(standing ** slope) + 1 for standing in range(1, number_of + 1)]
    largest = limit if full else min(limit, max(-(-total // number_of), total * weights[0] // sum(weights)))
    least = 1 if total - largest >= number_of - 1 else 0
    counts, rest = [largest] + [least] * (number_of - 1), total - largest - least * (number_of - 1)
    while rest > 0:
        movable = [i for i in range(1, number_of) if counts[i] < largest] or [i for i in range(1, number_of) if counts[i] < limit]
        whole, budget = sum([weights[i] for i in movable]), rest
        for i in movable:
            addition = min(limit - counts[i], max(1, budget * weights[i] // whole), rest)
            counts[i] = counts[i] + addition
            rest = rest - addition
    return np.array(counts)


def noise(stream_key, extent, spread, most, cuts=(), kind=jnp.bfloat16):
    gain = levels(stream_key, extent, cuts, -0.22, 0.18) if cuts else 1.0
    drawn = jax.random.normal(stream_key, extent, jnp.float32) * spread * gain
    return jnp.minimum(jnp.maximum(drawn, -most), most).astype(kind)


def setup_inputs(seed: int = 0) -> dict:
    key_of = jax.random.split(jax.random.key(seed), 7)
    samples = draw_samples(jax.random.fold_in(key_of[6], 71), 0)
    gate_weight = draw_gate_weight(jax.random.fold_in(key_of[6], 71), 0)
    expert_ids_keys = jax.random.split(jax.random.fold_in(key_of[2], 1), BATCH // ROWS_DEV)
    expert_ids_turns = jax.random.permutation(jax.random.fold_in(key_of[2], 3), BATCH // ROWS_DEV)
    expert_ids = jax.vmap(lambda own, number: routed_block(jax.random.fold_in(key_of[2], 2), own, number, ROWS_DEV, EXPERTS, 2, CAP, 1))(expert_ids_keys, expert_ids_turns).reshape((BATCH, 2))
    pad_mask = place_ends((jax.random.randint(key_of[3], (BATCH,), 0, 8) < 7).astype(jnp.int32), jax.random.fold_in(key_of[3], 1), 0, 1)
    up_weight = noise(key_of[4], (EXPERTS, D, H), D ** -0.5, 0.09375, ((0, 32),))
    down_weight = noise(key_of[5], (EXPERTS, H, OUT), H ** -0.5, 0.1875, ((0, 32),))
    return {"samples": samples, "gate_weight": gate_weight, "expert_ids": expert_ids, "pad_mask": pad_mask, "up_weight": up_weight, "down_weight": down_weight}


def reference(samples, gate_weight, expert_ids, pad_mask, up_weight, down_weight):
    logits = jnp.dot(samples, gate_weight, preferred_element_type=jnp.float32)
    row_top = jnp.max(logits, axis=1, keepdims=True)
    row_total = jnp.sum(jnp.exp(logits - row_top), axis=1, keepdims=True)
    chosen = jnp.take_along_axis(logits, expert_ids, axis=1)
    factor = EXPERTS * jnp.exp(chosen - row_top) / row_total * pad_mask.astype(jnp.float32)[:, None]
    grouped = expert_ids.reshape(N_EXPERT, ROWS_DEV * 2)
    onehot = (grouped[:, :, None] == jnp.arange(EXPERTS, dtype=jnp.int32)[None, None, :]).astype(jnp.int32)
    slot_rank = jnp.sum(onehot * (jnp.cumsum(onehot, axis=1) - 1), axis=2)
    source_index = jnp.arange(N_EXPERT, dtype=jnp.int32)[:, None]
    position = (grouped * (N_EXPERT * CAP) + source_index * CAP + slot_rank).reshape(-1).astype(jnp.int32)
    row_index = jnp.repeat(jnp.arange(BATCH, dtype=jnp.int32), 2)
    owners = jnp.full((EXPERTS * N_EXPERT * CAP,), BATCH, jnp.int32).at[position].set(row_index)
    padded = jnp.concatenate([samples, jnp.zeros((1, D), samples.dtype)], axis=0)

    def expert_pass(operands):
        owner_block, first, second = operands
        slot_block = padded[owner_block]
        hidden = jnp.dot(slot_block, first, preferred_element_type=jnp.float32)
        active = jnp.maximum(hidden, 0.0).astype(jnp.bfloat16)
        return jnp.dot(active, second, preferred_element_type=jnp.float32).astype(jnp.bfloat16)

    results = lax.map(expert_pass, (owners.reshape(EXPERTS, N_EXPERT * CAP), up_weight, down_weight))
    flat_out = results.reshape(EXPERTS * N_EXPERT * CAP, OUT)
    picked = flat_out[position].astype(jnp.float32).reshape(BATCH, 2, OUT)
    return jnp.sum(factor[:, :, None] * picked, axis=1).astype(jnp.bfloat16)
```

```python
import jax
import jax.numpy as jnp
from jax import lax
from jax.sharding import PartitionSpec as P


def peers(count, step):
    if count & (count - 1) == 0:
        return [(i, i ^ step) for i in range(count)]
    return [(i, (i + step) % count) for i in range(count)]


def owner_of(index, count, step):
    if count & (count - 1) == 0:
        return index ^ step
    return (index - step) % count


def per_device(samples, gate_weight, expert_ids, pad_mask, up_weight, down_weight):
    row_count, share = samples.shape
    group_count = lax.axis_size("expert")
    gate_count = lax.axis_size("gate")
    expert_count = group_count * gate_count
    capacity = 4 * row_count // expert_count
    gate_index = lax.axis_index("gate")

    shares = [samples]
    for step in range(1, gate_count):
        shares.append(lax.ppermute(samples, "gate", peers(gate_count, step)))

    ids = expert_ids.T
    experts = jnp.arange(expert_count, dtype=jnp.int32)
    named = ((ids[0][:, None] == experts) | (ids[1][:, None] == experts)).astype(jnp.bfloat16)
    rows = jnp.arange(row_count, dtype=jnp.int32)
    earlier = (rows[:, None] > rows[None, :]).astype(jnp.bfloat16)
    before = jnp.dot(earlier, named, preferred_element_type=jnp.float32)
    rank = jnp.sum(
        jnp.where(ids[:, :, None] == experts, before[None], 0.0), axis=2
    ).astype(jnp.int32)
    slot = ids * capacity + rank

    key = jnp.where(ids % gate_count == gate_index, ids // gate_count * capacity + rank, -1)
    column = jnp.arange(group_count * capacity, dtype=jnp.int32)[:, None]
    chooser = ((column == key[0][None, :]) | (column == key[1][None, :])).astype(jnp.bfloat16)

    partial_logits = lax.dot_general(
        gate_weight, samples, (((0,), (1,)), ((), ())), preferred_element_type=jnp.float32
    )
    logits = lax.psum(partial_logits, "gate")

    hidden = None
    for step in range(gate_count):
        outgoing = jnp.dot(
            chooser, shares[step], preferred_element_type=jnp.float32
        ).astype(jnp.bfloat16)
        incoming = lax.all_to_all(
            outgoing.reshape(group_count, capacity, share),
            "expert",
            split_axis=0,
            concat_axis=0,
            tiled=True,
        )
        weight = lax.dynamic_slice_in_dim(
            up_weight[0], owner_of(gate_index, gate_count, step) * share, share, 0
        )
        product = jnp.dot(
            incoming.reshape(group_count * capacity, share),
            weight,
            preferred_element_type=jnp.float32,
        )
        hidden = product if hidden is None else hidden + product
    active = jnp.maximum(hidden, 0.0).astype(jnp.bfloat16)
    expert_out = jnp.dot(active, down_weight[0], preferred_element_type=jnp.float32).astype(
        jnp.bfloat16
    )
    out_share = expert_out.shape[1] // gate_count
    outbound = expert_out.reshape(group_count, capacity, gate_count, out_share)
    outbound = outbound.transpose(0, 2, 1, 3).reshape(expert_count, capacity, out_share)
    returned = lax.all_to_all(
        outbound, ("expert", "gate"), split_axis=0, concat_axis=0, tiled=True
    ).reshape(expert_count * capacity, out_share)

    row_top = jnp.max(logits, axis=0)
    terms = jnp.exp(logits - row_top[None, :])
    row_total = jnp.sum(terms, axis=0)
    numerator = jnp.sum(
        jnp.where(ids[:, None, :] == experts[None, :, None], terms[None], 0.0), axis=1
    )
    factor = expert_count * numerator / row_total[None, :] * pad_mask.astype(jnp.float32)[None, :]

    every_slot = jnp.arange(expert_count * capacity, dtype=jnp.int32)
    picker = (slot.reshape(-1)[:, None] == every_slot[None, :]).astype(jnp.bfloat16)
    picked = jnp.dot(picker, returned, preferred_element_type=jnp.float32)
    mixed = factor[0][:, None] * picked[:row_count] + factor[1][:, None] * picked[row_count:]
    return mixed.astype(jnp.bfloat16)


def solution(mesh):
    placed = (
        P("expert", "gate"),
        P("gate", None),
        P("expert", None),
        P("expert"),
        P(("expert", "gate"), None, None),
        P(("expert", "gate"), None, None),
    )
    return jax.shard_map(
        per_device, mesh=mesh, in_specs=placed, out_specs=P("expert", "gate"), check_vma=False
    )
```

```python
import jax
import jax.numpy as jnp
from jax import lax
from jax.sharding import PartitionSpec as P


def peers(count, step):
    if count & (count - 1) == 0:
        return [(i, i ^ step) for i in range(count)]
    return [(i, (i + step) % count) for i in range(count)]


def owner_of(index, count, step):
    if count & (count - 1) == 0:
        return index ^ step
    return (index - step) % count


def per_device(samples, gate_weight, expert_ids, pad_mask, up_weight, down_weight):
    row_count, share = samples.shape
    group_count = lax.axis_size("expert")
    gate_count = lax.axis_size("gate")
    expert_count = group_count * gate_count
    capacity = 4 * row_count // expert_count
    gate_index = lax.axis_index("gate")

    shares = [samples]
    for step in range(1, gate_count):
        shares.append(lax.ppermute(samples, "gate", peers(gate_count, step)))

    ids = expert_ids.T
    experts = jnp.arange(expert_count, dtype=jnp.int32)
    named = ((ids[0][:, None] == experts) | (ids[1][:, None] == experts)).astype(jnp.bfloat16)
    rows = jnp.arange(row_count, dtype=jnp.int32)
    earlier = (rows[:, None] > rows[None, :]).astype(jnp.bfloat16)
    before = jnp.dot(earlier, named, preferred_element_type=jnp.float32)
    rank = jnp.sum(
        jnp.where(ids[:, :, None] == experts, before[None], 0.0), axis=2
    ).astype(jnp.int32)
    slot = (ids % gate_count * group_count + ids // gate_count) * capacity + rank

    key = jnp.where(ids % gate_count == gate_index, ids // gate_count * capacity + rank, -1)
    column = jnp.arange(group_count * capacity, dtype=jnp.int32)[:, None]
    chooser = ((column == key[0][None, :]) | (column == key[1][None, :])).astype(jnp.bfloat16)

    partial_logits = lax.dot_general(
        gate_weight, samples, (((0,), (1,)), ((), ())), preferred_element_type=jnp.float32
    )
    logits = lax.psum(partial_logits, "gate")

    chooser = lax.optimization_barrier(chooser)
    stages = stages_of(gate_count)
    hidden = None
    for stage, steps in enumerate(stages):
        picks = [
            jnp.dot(chooser, shares[step], preferred_element_type=jnp.float32)
            .astype(jnp.bfloat16)
            .reshape(group_count, 1, capacity, share)
            for step in steps
        ]
        outgoing = picks[0] if len(steps) == 1 else jnp.concatenate(picks, axis=1)
        incoming = lax.all_to_all(
            outgoing, "expert", split_axis=0, concat_axis=0, tiled=True
        )
        for place, step in enumerate(steps):
            weight = lax.dynamic_slice_in_dim(
                up_weight[0], owner_of(gate_index, gate_count, step) * share, share, 0
            )
            product = jnp.dot(
                incoming[:, place].reshape(group_count * capacity, share),
                weight,
                preferred_element_type=jnp.float32,
            )
            hidden = product if hidden is None else hidden + product
        if stage + 1 < len(stages):
            hidden = lax.optimization_barrier(hidden)
    active = jnp.maximum(hidden, 0.0).astype(jnp.bfloat16)
    out_share = down_weight.shape[2] // gate_count
    outbound = jnp.stack(
        [
            jnp.dot(
                active,
                down_weight[0, :, part * out_share : (part + 1) * out_share],
                preferred_element_type=jnp.float32,
            ).astype(jnp.bfloat16)
            for part in range(gate_count)
        ]
    ).reshape(expert_count, capacity, out_share)
    returned = lax.all_to_all(
        outbound, ("gate", "expert"), split_axis=0, concat_axis=0, tiled=True
    ).reshape(expert_count * capacity, out_share)

    row_top = jnp.max(logits, axis=0)
    terms = jnp.exp(logits - row_top[None, :])
    row_total = jnp.sum(terms, axis=0)
    numerator = jnp.sum(
        jnp.where(ids[:, None, :] == experts[None, :, None], terms[None], 0.0), axis=1
    )
    factor = expert_count * numerator / row_total[None, :] * pad_mask.astype(jnp.float32)[None, :]

    every_slot = jnp.arange(expert_count * capacity, dtype=jnp.int32)
    picker = (slot.reshape(-1)[:, None] == every_slot[None, :]).astype(jnp.bfloat16)
    picked = jnp.dot(picker, returned, preferred_element_type=jnp.float32)
    mixed = factor[0][:, None] * picked[:row_count] + factor[1][:, None] * picked[row_count:]
    return mixed.astype(jnp.bfloat16)


def stages_of(gate_count):
    if gate_count < 4:
        return [[step] for step in range(gate_count)]
    return [[0], list(range(1, gate_count - 1)), [gate_count - 1]]


def solution(mesh):
    placed = (
        P("expert", "gate"),
        P("gate", None),
        P("expert", None),
        P("expert"),
        P(("expert", "gate"), None, None),
        P(("expert", "gate"), None, None),
    )
    return jax.shard_map(
        per_device, mesh=mesh, in_specs=placed, out_specs=P("expert", "gate"), check_vma=False
    )
```

```python
import jax
import jax.numpy as jnp
from jax import lax
from jax.sharding import PartitionSpec as P


def peers(count, step):
    if count & (count - 1) == 0:
        return [(i, i ^ step) for i in range(count)]
    return [(i, (i + step) % count) for i in range(count)]


def owner_of(index, count, step):
    if count & (count - 1) == 0:
        return index ^ step
    return (index - step) % count


def hopped(turned, rows, group_count, capacity):
    own = lax.axis_index("expert")
    arrived = []
    for hop in range(group_count):
        piece = jnp.dot(
            turned[hop * capacity : (hop + 1) * capacity],
            rows,
            preferred_element_type=jnp.float32,
        ).astype(jnp.bfloat16)
        if hop:
            links = [(i, (i + hop) % group_count) for i in range(group_count)]
            piece = lax.ppermute(piece, "expert", links)
        arrived.append(piece)
    listed = [arrived[-place % group_count] for place in range(group_count)]
    twice = jnp.stack(listed + listed)
    return lax.dynamic_slice_in_dim(twice, group_count - own, group_count, 0)


def per_device(samples, gate_weight, expert_ids, pad_mask, up_weight, down_weight):
    row_count, share = samples.shape
    group_count = lax.axis_size("expert")
    gate_count = lax.axis_size("gate")
    expert_count = group_count * gate_count
    capacity = 4 * row_count // expert_count
    gate_index = lax.axis_index("gate")

    shares = [samples]
    for step in range(1, gate_count):
        shares.append(lax.ppermute(samples, "gate", peers(gate_count, step)))

    ids = expert_ids.T
    experts = jnp.arange(expert_count, dtype=jnp.int32)
    named = ((ids[0][:, None] == experts) | (ids[1][:, None] == experts)).astype(jnp.bfloat16)
    rows = jnp.arange(row_count, dtype=jnp.int32)
    earlier = (rows[:, None] > rows[None, :]).astype(jnp.bfloat16)
    before = jnp.dot(earlier, named, preferred_element_type=jnp.float32)
    rank = jnp.sum(
        jnp.where(ids[:, :, None] == experts, before[None], 0.0), axis=2
    ).astype(jnp.int32)
    slot = (ids % gate_count * group_count + ids // gate_count) * capacity + rank

    key = jnp.where(ids % gate_count == gate_index, ids // gate_count * capacity + rank, -1)
    column = jnp.arange(group_count * capacity, dtype=jnp.int32)[:, None]
    chooser = ((column == key[0][None, :]) | (column == key[1][None, :])).astype(jnp.bfloat16)

    partial_logits = lax.dot_general(
        gate_weight, samples, (((0,), (1,)), ((), ())), preferred_element_type=jnp.float32
    )
    logits = lax.psum(partial_logits, "gate")

    own = lax.axis_index("expert")
    ahead = jnp.where(
        ids % gate_count == gate_index,
        (ids // gate_count - own) % group_count * capacity + rank,
        -1,
    )
    turned = ((column == ahead[0][None, :]) | (column == ahead[1][None, :])).astype(jnp.bfloat16)
    chooser, turned = lax.optimization_barrier((chooser, turned))
    stages = stages_of(gate_count)
    hidden = None
    for stage, steps in enumerate(stages):
        if 0 < stage < len(stages) - 1:
            incoming = jnp.stack(
                [hopped(turned, shares[step], group_count, capacity) for step in steps], axis=1
            )
        else:
            picks = [
                jnp.dot(chooser, shares[step], preferred_element_type=jnp.float32)
                .astype(jnp.bfloat16)
                .reshape(group_count, 1, capacity, share)
                for step in steps
            ]
            outgoing = picks[0] if len(steps) == 1 else jnp.concatenate(picks, axis=1)
            incoming = lax.all_to_all(outgoing, "expert", split_axis=0, concat_axis=0, tiled=True)
        for place, step in enumerate(steps):
            weight = lax.dynamic_slice_in_dim(
                up_weight[0], owner_of(gate_index, gate_count, step) * share, share, 0
            )
            product = jnp.dot(
                incoming[:, place].reshape(group_count * capacity, share),
                weight,
                preferred_element_type=jnp.float32,
            )
            hidden = product if hidden is None else hidden + product
        if stage + 1 < len(stages):
            hidden = lax.optimization_barrier(hidden)
    active = jnp.maximum(hidden, 0.0).astype(jnp.bfloat16)
    out_share = down_weight.shape[2] // gate_count
    outbound = jnp.stack(
        [
            jnp.dot(
                active,
                down_weight[0, :, part * out_share : (part + 1) * out_share],
                preferred_element_type=jnp.float32,
            ).astype(jnp.bfloat16)
            for part in range(gate_count)
        ]
    ).reshape(expert_count, capacity, out_share)
    returned = lax.all_to_all(
        outbound, ("gate", "expert"), split_axis=0, concat_axis=0, tiled=True
    ).reshape(expert_count * capacity, out_share)

    row_top = jnp.max(logits, axis=0)
    terms = jnp.exp(logits - row_top[None, :])
    row_total = jnp.sum(terms, axis=0)
    numerator = jnp.sum(
        jnp.where(ids[:, None, :] == experts[None, :, None], terms[None], 0.0), axis=1
    )
    factor = expert_count * numerator / row_total[None, :] * pad_mask.astype(jnp.float32)[None, :]

    every_slot = jnp.arange(expert_count * capacity, dtype=jnp.int32)
    picker = (slot.reshape(-1)[:, None] == every_slot[None, :]).astype(jnp.bfloat16)
    picked = jnp.dot(picker, returned, preferred_element_type=jnp.float32)
    mixed = factor[0][:, None] * picked[:row_count] + factor[1][:, None] * picked[row_count:]
    return mixed.astype(jnp.bfloat16)


def stages_of(gate_count):
    if gate_count < 4:
        return [[step] for step in range(gate_count)]
    return [[0], list(range(1, gate_count - 1)), [gate_count - 1]]


def solution(mesh):
    placed = (
        P("expert", "gate"),
        P("gate", None),
        P("expert", None),
        P("expert"),
        P(("expert", "gate"), None, None),
        P(("expert", "gate"), None, None),
    )
    return jax.shard_map(
        per_device, mesh=mesh, in_specs=placed, out_specs=P("expert", "gate"), check_vma=False
    )
```
